32 devices in a mesh: dp: 1 (over z), sp: 32 (over y, x, core).
Axes of the slice: x: 4, y: 4, z: 1, core: 2. Of those that a mesh axis runs over, the one named last changes fastest.
The devices are a block of a 4x4x8 slice.
Arguments:
- resid: float32 [8, 2048, 2048], P('dp', 'sp')
- pre_norm: float32 [2, 2048], replicated
- w_in: bfloat16 [2, 2048, 8512], replicated
- conv_w: float32 [2, 4352, 4], replicated
- conv_b: float32 [2, 4352], replicated
- dt_bias: float32 [2, 64], replicated
- a_log: float32 [2, 64], replicated
- d_skip: float32 [2, 64], replicated
- gate_norm: float32 [2, 1, 4096], replicated
- w_out: bfloat16 [2, 4096, 2048], replicated
Outputs:
- output 1: float32 [8, 2048, 2048], P('dp', 'sp')
- output 2: float32 [8, 2, 64, 64, 128], P('dp', None, 'sp')
- output 3: bfloat16 [8, 2, 4352, 3], P('dp')
All inputs are finite; a program needn't handle non-finite values.
Results may differ from the reference program's by a relative error of at most 0.0188396.
Values are sent between devices in bfloat16 or wider.
A program may use at most 768 MiB of HBM per device.

```python
import jax
import jax.numpy as jnp
from jax import lax

D_MODEL = 2048
D_INNER = 4096
NUM_HEADS = 64
HEAD_DIM = 64
NUM_GROUPS = 1
D_STATE = 128
BATCH = 8
SEQ_LEN = 2048
LAYERS = 2
CONV_WIDTH = 4
CHUNK = 256

CONV_DIM = D_INNER + 2 * NUM_GROUPS * D_STATE
IN_DIM = D_INNER + CONV_DIM + NUM_HEADS
PER_GROUP = NUM_HEADS // NUM_GROUPS
GROUP_WIDTH = D_INNER // NUM_GROUPS
EPSILON = 1e-5


def setup_inputs(seed: int = 0, part: int = 0) -> dict:
    key = jax.random.key(seed)
    keys = jax.random.split(key, 9)
    part_key = jax.random.fold_in(key, part)
    resid = jax.random.normal(part_key, (BATCH, SEQ_LEN, D_MODEL), jnp.float32)
    pre_norm = jax.random.uniform(keys[0], (LAYERS, D_MODEL), jnp.float32, 0.5, 1.5)
    w_in = (jax.random.normal(keys[1], (LAYERS, D_MODEL, IN_DIM), jnp.float32) * D_MODEL ** -0.5).astype(jnp.bfloat16)
    bc_weight = 1.5 * (SEQ_LEN * D_STATE) ** -0.25
    column_scale = jnp.concatenate([jnp.full((D_INNER,), 0.5, jnp.float32), jnp.full((2 * NUM_GROUPS * D_STATE,), bc_weight, jnp.float32)])
    conv_w = jax.random.normal(keys[2], (LAYERS, CONV_DIM, CONV_WIDTH), jnp.float32) * column_scale[:, None]
    conv_b = jax.random.normal(keys[3], (LAYERS, CONV_DIM), jnp.float32) * 0.5 * column_scale
    dt_bias = jax.random.uniform(keys[4], (LAYERS, NUM_HEADS), jnp.float32, -1.0, 1.0)
    a_log = jnp.log(jax.random.uniform(keys[5], (LAYERS, NUM_HEADS), jnp.float32, 0.5, 2.0) / SEQ_LEN)
    d_skip = jax.random.uniform(keys[6], (LAYERS, NUM_HEADS), jnp.float32, 0.5, 1.5)
    gate_norm = jax.random.uniform(keys[7], (LAYERS, NUM_GROUPS, GROUP_WIDTH), jnp.float32, 0.5, 1.5)
    w_out = (jax.random.normal(keys[8], (LAYERS, D_INNER, D_MODEL), jnp.float32) * D_INNER ** -0.5).astype(jnp.bfloat16)
    return {'resid': resid, 'pre_norm': pre_norm, 'w_in': w_in, 'conv_w': conv_w, 'conv_b': conv_b, 'dt_bias': dt_bias, 'a_log': a_log, 'd_skip': d_skip, 'gate_norm': gate_norm, 'w_out': w_out}


def rms_norm(values, gain_vec):
    mean_sq = jnp.mean(values * values, axis=-1, keepdims=True)
    return values * lax.rsqrt(mean_sq + EPSILON) * gain_vec


def ssd_sequence(x_sequence, dt_sequence, b_sequence, c_sequence, a_neg):
    n_chunks = SEQ_LEN // CHUNK
    x_scaled = (x_sequence * dt_sequence[:, :, None]).reshape(n_chunks, CHUNK, NUM_GROUPS, PER_GROUP, HEAD_DIM)
    log_decay = (dt_sequence * a_neg).reshape(n_chunks, CHUNK, NUM_GROUPS, PER_GROUP)
    b_chunks = b_sequence.reshape(n_chunks, CHUNK, NUM_GROUPS, D_STATE)
    c_chunks = c_sequence.reshape(n_chunks, CHUNK, NUM_GROUPS, D_STATE)
    causal = jnp.arange(CHUNK)[:, None] >= jnp.arange(CHUNK)[None, :]

    def chunk_step(state, chunk_data):
        x_chunk, log_chunk, b_chunk, c_chunk = chunk_data
        cum_log = jnp.cumsum(log_chunk, axis=0)
        cum_heads = jnp.transpose(cum_log, (1, 2, 0))
        log_diff = cum_heads[:, :, :, None] - cum_heads[:, :, None, :]
        decay_mat = jnp.exp(jnp.where(causal, log_diff, -jnp.inf))
        scores = jnp.einsum('tgn,sgn->gts', c_chunk, b_chunk)
        mix_mat = decay_mat * scores[:, None]
        y_intra = jnp.einsum('ghts,sghp->tghp', mix_mat, x_chunk)
        y_inter = jnp.einsum('tgn,ghpn->tghp', c_chunk, state) * jnp.exp(cum_log)[:, :, :, None]
        to_end = jnp.exp(cum_log[-1] - cum_log)
        new_state = state * jnp.exp(cum_log[-1])[:, :, None, None] + jnp.einsum('sghp,sgn->ghpn', x_chunk * to_end[:, :, :, None], b_chunk)
        return new_state, y_intra + y_inter

    state_zero = jnp.zeros((NUM_GROUPS, PER_GROUP, HEAD_DIM, D_STATE), jnp.float32)
    final, y_chunks = lax.scan(chunk_step, state_zero, (x_scaled, log_decay, b_chunks, c_chunks))
    return y_chunks.reshape(SEQ_LEN, NUM_HEADS, HEAD_DIM), final.reshape(NUM_HEADS, HEAD_DIM, D_STATE)


def mamba_layer(resid, pre_w, w_in_l, conv_w_l, conv_b_l, dt_b, a_log_l, d_l, gate_w, w_out_l):
    normed = rms_norm(resid, pre_w).astype(jnp.bfloat16)
    projected = jnp.dot(normed.reshape(-1, D_MODEL), w_in_l, preferred_element_type=jnp.float32).astype(jnp.bfloat16).reshape(BATCH, SEQ_LEN, IN_DIM)
    gate_z = projected[:, :, :D_INNER]
    xbc = projected[:, :, D_INNER:D_INNER + CONV_DIM]
    dt_raw = projected[:, :, D_INNER + CONV_DIM:]
    padded = jnp.pad(xbc, ((0, 0), (CONV_WIDTH - 1, 0), (0, 0))).astype(jnp.float32)
    conv_out = conv_b_l + sum(padded[:, tap_index:tap_index + SEQ_LEN] * conv_w_l[:, tap_index] for tap_index in range(CONV_WIDTH))
    activated = jax.nn.silu(conv_out).astype(jnp.bfloat16)
    x_act = activated[:, :, :D_INNER].reshape(BATCH, SEQ_LEN, NUM_HEADS, HEAD_DIM)
    b_act = activated[:, :, D_INNER:D_INNER + NUM_GROUPS * D_STATE].reshape(BATCH, SEQ_LEN, NUM_GROUPS, D_STATE)
    c_act = activated[:, :, D_INNER + NUM_GROUPS * D_STATE:].reshape(BATCH, SEQ_LEN, NUM_GROUPS, D_STATE)
    delta = jax.nn.softplus(dt_raw.astype(jnp.float32) + dt_b).astype(jnp.bfloat16)
    a_neg = -jnp.exp(a_log_l)

    def one_sequence(seq_parts):
        x_part, dt_part, b_part, c_part = seq_parts
        return ssd_sequence(x_part.astype(jnp.float32), dt_part.astype(jnp.float32), b_part.astype(jnp.float32), c_part.astype(jnp.float32), a_neg)

    y_ssm, final = lax.map(one_sequence, (x_act, delta, b_act, c_act))
    y_full = (y_ssm + d_l[:, None] * x_act.astype(jnp.float32)).astype(jnp.bfloat16)
    gated = y_full.astype(jnp.float32).reshape(BATCH, SEQ_LEN, D_INNER) * jax.nn.silu(gate_z.astype(jnp.float32))
    grouped = gated.reshape(BATCH, SEQ_LEN, NUM_GROUPS, GROUP_WIDTH)
    normed_y = (grouped * lax.rsqrt(jnp.mean(grouped * grouped, axis=-1, keepdims=True) + EPSILON) * gate_w).astype(jnp.bfloat16)
    out_proj = jnp.dot(normed_y.reshape(-1, D_INNER), w_out_l, preferred_element_type=jnp.float32).reshape(BATCH, SEQ_LEN, D_MODEL)
    tail_rows = jnp.swapaxes(xbc[:, SEQ_LEN - (CONV_WIDTH - 1):], 1, 2)
    return resid + out_proj, final, tail_rows


def reference(resid, pre_norm, w_in, conv_w, conv_b, dt_bias, a_log, d_skip, gate_norm, w_out):
    def layer_step(carry, layer_weights):
        pre_w, w_in_l, conv_w_l, conv_b_l, dt_b, a_log_l, d_l, gate_w, w_out_l = layer_weights
        new_resid, final, tail_rows = mamba_layer(carry, pre_w, w_in_l, conv_w_l, conv_b_l, dt_b, a_log_l, d_l, gate_w, w_out_l)
        return new_resid, (final, tail_rows)

    out_resid, (finals, tails) = lax.scan(layer_step, resid, (pre_norm, w_in, conv_w, conv_b, dt_bias, a_log, d_skip, gate_norm, w_out))
    return out_resid, jnp.swapaxes(finals, 0, 1), jnp.swapaxes(tails, 0, 1)
```

```python
import functools

import jax
import jax.numpy as jnp
from jax import lax
from jax.experimental import pallas as pl
from jax.experimental.pallas import tpu as pltpu
from jax.sharding import PartitionSpec as P


CONV_WIDTH = 4
EPSILON = 1e-5
PROMPT_GROUPS = 2
HALO = 8
LANES = 128
NT = (((1,), (1,)), ((), ()))
X_TILE = 512
Z_TILE = 512
OUT_TILE = 512


def silu(values):
    return values * (1.0 / (1.0 + jnp.exp(-values)))


def pick_tile(preferred, total):
    tile = preferred
    while total % tile:
        tile //= 2
    return tile


def xbc_kernel(n_prompts, seg_len, d_inner, d_bc, n_heads, h_ref, halo_ref, w_ref, cw_ref, cb_ref, dtb_ref,
               xs_ref, bc_ref, tail_ref, h_ext, window, turned, dt_rows):
    step = pl.program_id(0)
    rows = n_prompts * seg_len
    tile = w_ref.shape[1]
    pair = LANES // seg_len
    dests = n_heads // pair

    @pl.when(step == 0)
    def _():
        h_ext[:rows] = h_ref[...]
        h_ext[rows:] = halo_ref[...]
        dt_rows[...] = jnp.zeros_like(dt_rows)

    projected = lax.dot_general(h_ext[...], w_ref[0], NT, preferred_element_type=jnp.float32).astype(jnp.bfloat16).astype(jnp.float32)
    window[:, HALO:, :] = projected[:rows].reshape(n_prompts, seg_len, tile)
    window[:, :HALO, :] = projected[rows:].reshape(n_prompts, HALO, tile)
    tail_ref[...] = window[:, seg_len:, :].astype(jnp.bfloat16)

    def convolve(prompt, lane_start, col_start):
        lanes = pl.ds(lane_start, LANES)
        acc = cb_ref[:, pl.ds(col_start, LANES)]
        for tap in range(CONV_WIDTH):
            first = HALO - (CONV_WIDTH - 1) + tap
            acc = acc + window[prompt, first:first + seg_len, lanes] * cw_ref[tap:tap + 1, pl.ds(col_start, LANES)]
        return silu(acc).astype(jnp.bfloat16)

    @pl.when(step == 0)
    def _():
        @pl.loop(0, n_prompts)
        def _(prompt):
            at = pl.ds(pl.multiple_of(prompt * seg_len, seg_len), seg_len)
            for start in range(0, d_bc, LANES):
                bc_ref[at, start:start + LANES] = convolve(prompt, start, d_inner + start)
            raw = window[prompt, HALO:, d_bc:d_bc + LANES] + dtb_ref[...]
            delta = jnp.maximum(raw, 0.0) + jnp.log1p(jnp.exp(-jnp.abs(raw)))
            delta = delta.astype(jnp.bfloat16).astype(jnp.float32)
            turned[...] = jnp.transpose(delta, (1, 0))
            parts = [turned[pl.ds(which, dests, stride=pair), :] for which in range(pair)]
            dt_rows[pl.ds(prompt, dests, stride=HALO), :] = jnp.concatenate(parts, axis=1)

    @pl.when(step > 0)
    def _():
        base = (step - 1) * tile

        @pl.loop(0, n_prompts)
        def _(prompt):
            at = pl.ds(pl.multiple_of(prompt * seg_len, seg_len), seg_len)
            for block in range(tile // LANES):
                start = block * LANES
                xs_ref[block, at, :] = convolve(prompt, start, pl.multiple_of(base + start, LANES))

        for block in range(tile // LANES):
            dest = (step - 1) * (tile // LANES) + block
            xs_ref[block, rows:, :] = dt_rows[pl.ds(pl.multiple_of(dest * HALO, HALO), HALO), :].astype(jnp.bfloat16)


def project_xbc(layer, h, halo, w_in, conv_w, conv_b, dt_bias, n_prompts, seg_len, d_inner, d_bc):
    rows, d_model = h.shape
    n_heads = dt_bias.shape[-1]
    conv_dim = d_inner + d_bc
    tile = pick_tile(X_TILE, d_inner)
    blocks = d_inner // LANES
    x_steps = d_inner // tile
    per = tile // LANES
    m_rows = rows + halo.shape[0]
    bias = jnp.pad(dt_bias[layer][None, :], ((0, 0), (0, LANES - n_heads)))
    x_block = lambda s: jnp.maximum(s - 1, 0)
    col = lambda s: jnp.where(s == 0, x_steps, s - 1)
    whole = lambda *shape: pl.BlockSpec(shape, lambda s: (0,) * len(shape))
    return pl.pallas_call(
        functools.partial(xbc_kernel, n_prompts, seg_len, d_inner, d_bc, n_heads),
        grid=(x_steps + 1,),
        in_specs=[whole(rows, d_model), whole(*halo.shape),
                  pl.BlockSpec((1, tile, d_model), lambda s: (layer, d_inner // tile + col(s), 0)),
                  whole(CONV_WIDTH, conv_dim), whole(1, conv_dim), whole(1, LANES)],
        out_specs=[pl.BlockSpec((per, rows + HALO, LANES), lambda s: (x_block(s), 0, 0)),
                   whole(rows, d_bc),
                   pl.BlockSpec((n_prompts, HALO, tile), lambda s: (0, 0, col(s)))],
        out_shape=[jax.ShapeDtypeStruct((blocks, rows + HALO, LANES), jnp.bfloat16),
                   jax.ShapeDtypeStruct((rows, d_bc), jnp.bfloat16),
                   jax.ShapeDtypeStruct((n_prompts, HALO, conv_dim), jnp.bfloat16)],
        scratch_shapes=[pltpu.VMEM((m_rows, d_model), jnp.bfloat16),
                        pltpu.VMEM((n_prompts, seg_len + HALO, tile), jnp.float32),
                        pltpu.VMEM((LANES, seg_len), jnp.float32),
                        pltpu.VMEM((blocks * HALO, LANES), jnp.float32)],
        cost_estimate=pl.CostEstimate(flops=2 * m_rows * d_model * (conv_dim + n_heads), bytes_accessed=2 * d_model * (conv_dim + n_heads), transcendentals=0),
    )(h, halo, w_in, conv_w, conv_b, bias)


def z_kernel(h_ref, w_ref, z_ref):
    z_ref[...] = lax.dot_general(h_ref[...], w_ref[0], NT, preferred_element_type=jnp.float32).astype(jnp.bfloat16)


def project_z(layer, h, w_in, d_inner):
    rows, d_model = h.shape
    tile = pick_tile(Z_TILE, d_inner)
    return pl.pallas_call(
        z_kernel,
        grid=(d_inner // tile,),
        in_specs=[pl.BlockSpec((rows, d_model), lambda s: (0, 0)),
                  pl.BlockSpec((1, tile, d_model), lambda s: (layer, s, 0))],
        out_specs=pl.BlockSpec((rows, tile), lambda s: (0, s)),
        out_shape=jax.ShapeDtypeStruct((rows, d_inner), jnp.bfloat16),
        cost_estimate=pl.CostEstimate(flops=2 * rows * d_model * d_inner, bytes_accessed=2 * d_model * d_inner, transcendentals=0),
    )(h, w_in)


def scan_kernel(n_prompts, seg_len, segs, head_dim, d_state, x_ref, bc_ref, a_ref, d_ref, y_ref, state_ref,
                row_refs, col_ref, dtc_ref):
    chunk = segs * seg_len
    rows = n_prompts * seg_len
    heads = LANES // head_dim

    @pl.when(pl.program_id(0) == 0)
    def _():
        state_ref[...] = jnp.zeros_like(state_ref)

    token_r = lax.broadcasted_iota(jnp.int32, (chunk, chunk), 0)
    token_c = lax.broadcasted_iota(jnp.int32, (chunk, chunk), 1)
    causal = token_r >= token_c
    lower = causal.astype(jnp.float32)
    upper = (token_r <= token_c).astype(jnp.float32)
    eye = (token_r == token_c).astype(jnp.float32)
    nt = (((1,), (1,)), ((), ()))
    tn = (((0,), (0,)), ((), ()))

    per_seg = [x_ref[seg, rows:, :].astype(jnp.float32) for seg in range(segs)]
    steps = jnp.concatenate([jnp.concatenate([part[:, head * seg_len:(head + 1) * seg_len] for part in per_seg], axis=1)
                             for head in range(heads)], axis=0)
    row_refs[...] = jnp.dot(steps, upper, preferred_element_type=jnp.float32)
    col_ref[...] = lax.dot_general(lower, steps, nt, preferred_element_type=jnp.float32)
    dtc_ref[...] = lax.dot_general(eye, steps, nt, preferred_element_type=jnp.float32)

    lane = lax.broadcasted_iota(jnp.int32, (chunk, LANES), 1)
    state_row = lax.broadcasted_iota(jnp.int32, (LANES, d_state), 0)
    pick = lax.broadcasted_iota(jnp.int32, (chunk, heads * HALO), 1)

    @pl.loop(0, n_prompts)
    def _(prompt):
        at = pl.ds(pl.multiple_of(prompt * seg_len, seg_len), seg_len)
        x_float = x_ref[:, at, :].reshape(chunk, LANES).astype(jnp.float32)
        b_part = bc_ref[:, at, :d_state].reshape(chunk, d_state)
        c_part = bc_ref[:, at, d_state:].reshape(chunk, d_state)
        scores = lax.dot_general(c_part, b_part, nt, preferred_element_type=jnp.float32)
        state = state_ref[prompt]
        y_inter = lax.dot_general(c_part.astype(jnp.float32), state, nt, preferred_element_type=jnp.float32)

        cums = [jnp.sum(jnp.where(pick == head * HALO + prompt, col_ref[...], 0.0), axis=1, keepdims=True) for head in range(heads)]
        dts = [jnp.sum(jnp.where(pick == head * HALO + prompt, dtc_ref[...], 0.0), axis=1, keepdims=True) for head in range(heads)]
        cum_log = jnp.broadcast_to(cums[0] * a_ref[0], (chunk, LANES))
        delta = jnp.broadcast_to(dts[0], (chunk, LANES))
        for head in range(1, heads):
            cum_log = jnp.where(lane >= head * head_dim, cums[head] * a_ref[head], cum_log)
            delta = jnp.where(lane >= head * head_dim, dts[head], delta)
        x_scaled = x_float * delta
        skip = jnp.broadcast_to(d_ref[0], (chunk, LANES))
        for head in range(1, heads):
            skip = jnp.where(lane >= head * head_dim, d_ref[head], skip)

        y_value = y_inter * jnp.exp(cum_log) + skip * x_float
        kept = jnp.zeros((LANES, d_state), jnp.float32)
        for head in range(heads):
            row = row_refs[pl.ds(head * HALO + prompt, 1), :]
            decay = jnp.exp(jnp.where(causal, (cums[head] - row) * a_ref[head], -jnp.inf))
            mine = (lane >= head * head_dim) & (lane < (head + 1) * head_dim)
            y_value = y_value + jnp.dot(decay * scores, jnp.where(mine, x_scaled, 0.0), preferred_element_type=jnp.float32)
            last = jnp.exp(cums[head][chunk - 1:chunk] * a_ref[head])
            kept = jnp.where(state_row >= head * head_dim, last, kept)
        x_left = x_scaled * jnp.exp(cum_log[chunk - 1:chunk] - cum_log)
        state_ref[prompt] = state * kept + lax.dot_general(x_left, b_part.astype(jnp.float32), tn, preferred_element_type=jnp.float32)
        y_ref[:, at, :] = y_value.astype(jnp.bfloat16).reshape(segs, seg_len, LANES)


def scan_heads(x_recv, bc_all, a_neg, d_vec, n_prompts, seg_len, head_dim, d_state):
    seg_count, rows_x, _ = x_recv.shape
    rows = n_prompts * seg_len
    heads = LANES // head_dim
    segs = 4
    while seg_count % segs:
        segs //= 2
    chunk = segs * seg_len
    steps = seg_count // segs
    flops = steps * n_prompts * 2 * chunk * LANES * (chunk * (1 + heads) + 2 * d_state)
    return pl.pallas_call(
        functools.partial(scan_kernel, n_prompts, seg_len, segs, head_dim, d_state),
        grid=(steps,),
        in_specs=[pl.BlockSpec((segs, rows_x, LANES), lambda s: (s, 0, 0)),
                  pl.BlockSpec((segs, rows, 2 * d_state), lambda s: (s, 0, 0)),
                  pl.BlockSpec(memory_space=pltpu.SMEM),
                  pl.BlockSpec(memory_space=pltpu.SMEM)],
        out_specs=[pl.BlockSpec((segs, rows, LANES), lambda s: (s, 0, 0)),
                   pl.BlockSpec((n_prompts, LANES, d_state), lambda s: (0, 0, 0))],
        out_shape=[jax.ShapeDtypeStruct((seg_count, rows, LANES), jnp.bfloat16),
                   jax.ShapeDtypeStruct((n_prompts, LANES, d_state), jnp.float32)],
        scratch_shapes=[pltpu.VMEM((heads * HALO, chunk), jnp.float32),
                        pltpu.VMEM((chunk, heads * HALO), jnp.float32),
                        pltpu.VMEM((chunk, heads * HALO), jnp.float32)],
        cost_estimate=pl.CostEstimate(flops=flops * 4, bytes_accessed=seg_count * rows * 2 * (2 * LANES + 2 * d_state), transcendentals=0),
    )(x_recv, bc_all, a_neg, d_vec)


def out_kernel(with_next, n_tiles, y_ref, z_ref, gate_ref, w_ref, resid_ref, pre_ref, *rest):
    if with_next:
        out_ref, h_ref, normed, gated, kept = rest
    else:
        out_ref, normed, gated = rest[-3:]
    step = pl.program_id(0)
    blocks, rows, _ = y_ref.shape
    part = gated.shape[0]
    tile = out_ref.shape[-1]

    @pl.when(step == 0)
    def _():
        @pl.loop(0, rows // part)
        def _(index):
            at = pl.ds(pl.multiple_of(index * part, part), part)
            total = jnp.zeros((part, LANES), jnp.float32)
            for block in range(blocks):
                lanes = slice(block * LANES, (block + 1) * LANES)
                value = y_ref[block, at, :].astype(jnp.float32) * silu(z_ref[at, lanes].astype(jnp.float32))
                total = total + value * value
                gated[:, lanes] = value
            mean_sq = jnp.sum(total, axis=1, keepdims=True) * (1.0 / (blocks * LANES))
            scale = lax.rsqrt(mean_sq + EPSILON)
            for block in range(blocks):
                lanes = slice(block * LANES, (block + 1) * LANES)
                normed[at, lanes] = (gated[:, lanes] * scale * gate_ref[:, lanes]).astype(jnp.bfloat16)

    value = resid_ref[...] + jnp.dot(normed[...], w_ref[0], preferred_element_type=jnp.float32)
    out_ref[...] = value
    if with_next:
        kept[:, pl.ds(pl.multiple_of(step * tile, tile), tile)] = value

        @pl.when(step == n_tiles - 1)
        def _():
            @pl.loop(0, rows // part)
            def _(index):
                at = pl.ds(pl.multiple_of(index * part, part), part)
                row = kept[at, :]
                mean_sq = jnp.mean(row * row, axis=1, keepdims=True)
                h_ref[at, :] = (row * lax.rsqrt(mean_sq + EPSILON) * pre_ref[...]).astype(jnp.bfloat16)


def project_out(layer, y_recv, z, gate_w, w_out, resid, resid_block, next_pre, shared=None, out_block=0, out_rows=None):
    blocks, rows, _ = y_recv.shape
    d_inner = blocks * LANES
    d_model = resid.shape[-1]
    tile = pick_tile(OUT_TILE, d_model)
    n_tiles = d_model // tile
    with_next = next_pre is not None
    part = min(32, rows)
    whole = lambda *shape: pl.BlockSpec(shape, lambda s: (0,) * len(shape), pipeline_mode=pl.Buffered(1))
    out_specs = [pl.BlockSpec((rows, tile), lambda s: (out_block, s))]
    out_shape = [jax.ShapeDtypeStruct((out_rows or rows, d_model), jnp.float32)]
    scratch = [pltpu.VMEM((rows, d_inner), jnp.bfloat16), pltpu.VMEM((part, d_inner), jnp.float32)]
    if with_next:
        out_specs.append(pl.BlockSpec((rows, d_model), lambda s: (0, 0)))
        out_shape.append(jax.ShapeDtypeStruct((rows, d_model), jnp.bfloat16))
        scratch.append(pltpu.VMEM((rows, d_model), jnp.float32))
    else:
        next_pre = gate_w[:, :d_model]
    extra = [] if shared is None else [shared]
    result = pl.pallas_call(
        functools.partial(out_kernel, with_next, n_tiles),
        grid=(n_tiles,),
        in_specs=[whole(blocks, rows, LANES), whole(rows, d_inner), whole(1, d_inner),
                  pl.BlockSpec((1, d_inner, tile), lambda s: (layer, 0, s)),
                  pl.BlockSpec((rows, tile), lambda s: (resid_block, s)), whole(1, d_model)] + [pl.BlockSpec(memory_space=pl.ANY)] * len(extra),
        input_output_aliases={6: 0} if extra else {},
        out_specs=out_specs,
        out_shape=out_shape,
        scratch_shapes=scratch,
        cost_estimate=pl.CostEstimate(flops=2 * rows * d_inner * d_model, bytes_accessed=2 * d_inner * d_model, transcendentals=0),
    )(y_recv, z, gate_w, w_out, resid, next_pre, *extra)
    return (result[0], result[1]) if with_next else (result[0], None)


def solution(mesh):
    seg_count = mesh.shape['sp']

    def step(resid, pre_norm, w_in, conv_w, conv_b, dt_bias, a_log, d_skip, gate_norm, w_out):
        batch, seg_len, d_model = resid.shape
        n_layers, n_groups, group_width = gate_norm.shape
        d_inner = n_groups * group_width
        n_heads = dt_bias.shape[1]
        conv_dim = conv_b.shape[1]
        d_bc = conv_dim - d_inner
        d_state = d_bc // (2 * n_groups)
        head_dim = d_inner // n_heads
        local_heads = n_heads // seg_count
        assert n_groups == 1 and local_heads * head_dim == LANES
        seg_index = lax.axis_index('sp')
        n_prompts = batch // PROMPT_GROUPS
        rows = n_prompts * seg_len
        taps = jnp.swapaxes(conv_w, 1, 2)
        a_neg = -jnp.exp(lax.dynamic_slice_in_dim(a_log, seg_index * local_heads, local_heads, axis=1))
        d_local = lax.dynamic_slice_in_dim(d_skip, seg_index * local_heads, local_heads, axis=1)
        hops = [(source, source + 1) for source in range(seg_count - 1)]

        w_rows = jnp.swapaxes(w_in, 1, 2)
        whole_resid = resid.reshape(batch * seg_len, d_model)
        streams = []
        for group in range(PROMPT_GROUPS):
            part = whole_resid[group * rows:(group + 1) * rows]
            mean_sq = jnp.mean(part * part, axis=-1, keepdims=True)
            h = (part * lax.rsqrt(mean_sq + EPSILON) * pre_norm[0]).astype(jnp.bfloat16)
            streams.append((whole_resid, group, h))

        finals = []
        tails = []
        summed = None
        for layer in range(n_layers):
            final_layer = layer + 1 == n_layers
            layer_finals = []
            sent = []
            for _, _, h in streams:
                edge = h.reshape(n_prompts, seg_len, d_model)[:, seg_len - HALO:].reshape(n_prompts * HALO, d_model)
                halo = lax.ppermute(edge, 'sp', hops)
                sent.append(project_xbc(layer, h, halo, w_rows, taps[layer], conv_b[layer][None, :], dt_bias, n_prompts, seg_len, d_inner, d_bc))
            tail = jnp.concatenate([item[2][:, HALO - (CONV_WIDTH - 1):] for item in sent], axis=0)
            tail = jnp.where(seg_index == seg_count - 1, tail, jnp.zeros((), jnp.bfloat16)).reshape(batch * (CONV_WIDTH - 1), conv_dim)
            if summed is not None:
                tail, summed = lax.optimization_barrier((tail, summed))
                tails[-1] = summed
            summed = lax.optimization_barrier(lax.psum(tail, 'sp'))
            tails.append(summed)
            gates = []
            arrived = []
            for group, (_, _, h) in enumerate(streams):
                x_send, bc, _ = sent[group]
                x_recv = lax.all_to_all(x_send, 'sp', 0, 0, tiled=True)
                bc_all = lax.all_gather(bc, 'sp', axis=0)
                arrived.append((x_recv, bc_all))
                gates.append(project_z(layer, h, w_rows, d_inner))
            next_streams = []
            shared = None
            for group, (part, block, h) in enumerate(streams):
                x_recv, bc_all = arrived[group]
                if group == 0:
                    bc_all, tail = lax.optimization_barrier((bc_all, tail))
                y_send, final = scan_heads(x_recv, bc_all, a_neg[layer], d_local[layer], n_prompts, seg_len, head_dim, d_state)
                layer_finals.append(final.reshape(n_prompts, local_heads, head_dim, d_state))
                y_recv = lax.all_to_all(y_send, 'sp', 0, 0, tiled=True)
                if final_layer:
                    shared, _ = project_out(layer, y_recv, gates[group], gate_norm[layer], w_out, part, block, None, shared, group, batch * seg_len)
                else:
                    new_part, new_h = project_out(layer, y_recv, gates[group], gate_norm[layer], w_out, part, block, pre_norm[layer + 1][None, :])
                    next_streams.append((new_part, 0, new_h))
            streams = next_streams
            finals.append(jnp.concatenate(layer_finals, axis=0))
        states = [jnp.swapaxes(tail.reshape(batch, CONV_WIDTH - 1, conv_dim), 1, 2) for tail in tails]
        return shared.reshape(batch, seg_len, d_model), jnp.stack(finals, axis=1), jnp.stack(states, axis=1)

    return jax.shard_map(step, mesh=mesh, in_specs=(P('dp', 'sp', None), P(), P(), P(), P(), P(), P(), P(), P(), P()), out_specs=(P('dp', 'sp', None), P('dp', None, 'sp', None, None), P('dp', None, None, None)), check_vma=False)
```

```python
import functools

import jax
import jax.numpy as jnp
from jax import lax
from jax.experimental import pallas as pl
from jax.experimental.pallas import tpu as pltpu
from jax.sharding import PartitionSpec as P


CONV_WIDTH = 4
EPSILON = 1e-5
PROMPT_GROUPS = 2
HALO = 8
PACK = 16
LANES = 128
SCAN_UNROLL = 2
NT = (((1,), (1,)), ((), ()))
X_TILE = 512
Z_TILE = 512
OUT_TILE = 512


def silu(values):
    return values * (1.0 / (1.0 + jnp.exp(-values)))


def pick_tile(preferred, total):
    tile = preferred
    while total % tile:
        tile //= 2
    return tile


def start_weights(w_ref, layer, first, tile, buffer, arrived):
    for index in range(buffer.shape[0]):
        pltpu.make_async_copy(w_ref.at[layer, pl.ds(first + index * tile, tile)], buffer.at[index], arrived.at[index]).start()


def wait_weights(w_ref, layer, first, tile, buffer, arrived, index):
    at = pl.ds(pl.multiple_of(first + index * tile, LANES), tile)
    pltpu.make_async_copy(w_ref.at[layer, at], buffer.at[index], arrived.at[index]).wait()


def fill_window(projected, window, n_prompts, seg_len):
    rows = n_prompts * seg_len
    width = window.shape[-1]
    window[:, HALO:, :] = projected[:rows].reshape(n_prompts, seg_len, width)
    window[:, :HALO, :] = projected[rows:].reshape(n_prompts, HALO, width)


def convolve(window, cw_ref, cb_ref, prompt, seg_len, lane_start, col_start):
    acc = cb_ref[:, pl.ds(col_start, LANES)]
    for tap in range(CONV_WIDTH):
        first = HALO - (CONV_WIDTH - 1) + tap
        acc = acc + window[prompt, first:first + seg_len, lane_start:lane_start + LANES] * cw_ref[tap:tap + 1, pl.ds(col_start, LANES)]
    return silu(acc).astype(jnp.bfloat16)


def rounded_product(left, right_rows):
    return lax.dot_general(left, right_rows, NT, preferred_element_type=jnp.float32).astype(jnp.bfloat16).astype(jnp.float32)


def bc_kernel(layer, n_prompts, seg_len, d_inner, d_bc, n_heads, h_ref, halo_ref, w_ref, cw_ref, cb_ref, dtb_ref,
              bc_ref, dt_ref, weights, arrived, h_ext, window, turned, dt_rows, last_rows):
    rows = n_prompts * seg_len
    pair = LANES // seg_len
    dests = n_heads // pair
    first = 2 * d_inner
    start_weights(w_ref, layer, first, d_bc + n_heads, weights, arrived)
    h_ext[:rows] = h_ref[...]
    h_ext[rows:] = halo_ref[...]
    dt_rows[...] = jnp.zeros_like(dt_rows)
    wait_weights(w_ref, layer, first, d_bc + n_heads, weights, arrived, 0)
    fill_window(rounded_product(h_ext[...], weights[0]), window, n_prompts, seg_len)
    per = CONV_WIDTH
    for prompt in range(n_prompts):
        at = slice(prompt * seg_len, (prompt + 1) * seg_len)
        last_rows[prompt * per:(prompt + 1) * per, :] = window[prompt, HALO + seg_len - per:, :d_bc]
        for start in range(0, d_bc, LANES):
            bc_ref[at, start:start + LANES] = convolve(window, cw_ref, cb_ref, prompt, seg_len, start, d_inner + start)
        raw = window[prompt, HALO:, d_bc:d_bc + n_heads] + dtb_ref[:, :n_heads]
        delta = jnp.maximum(raw, 0.0) + jnp.log1p(jnp.exp(-jnp.abs(raw)))
        delta = delta.astype(jnp.bfloat16).astype(jnp.float32)
        turned[...] = jnp.transpose(delta, (1, 0))
        parts = [turned[pl.ds(which, dests, stride=pair), :] for which in range(pair)]
        dt_rows[pl.ds(prompt, dests, stride=PACK), :] = jnp.concatenate(parts, axis=1)
    bc_ref[rows:, :] = last_rows[...].astype(jnp.bfloat16)
    dt_ref[...] = dt_rows[...].astype(jnp.bfloat16)


def project_bc(layer, h, halo, w_rows, conv_w, conv_b, dt_bias, n_prompts, seg_len, d_inner, d_bc):
    rows, d_model = h.shape
    n_heads = dt_bias.shape[-1]
    dests = d_inner // LANES
    m_rows = rows + halo.shape[0]
    vmem = pl.BlockSpec(memory_space=pltpu.VMEM)
    return pl.pallas_call(
        functools.partial(bc_kernel, layer, n_prompts, seg_len, d_inner, d_bc, n_heads),
        in_specs=[vmem, vmem, pl.BlockSpec(memory_space=pl.ANY), vmem, vmem, vmem],
        out_specs=[vmem, vmem],
        out_shape=[jax.ShapeDtypeStruct((rows + n_prompts * CONV_WIDTH, d_bc), jnp.bfloat16),
                   jax.ShapeDtypeStruct((dests * PACK, LANES), jnp.bfloat16)],
        scratch_shapes=[pltpu.VMEM((1, d_bc + n_heads, d_model), jnp.bfloat16),
                        pltpu.SemaphoreType.DMA((1,)),
                        pltpu.VMEM((m_rows, d_model), jnp.bfloat16),
                        pltpu.VMEM((n_prompts, seg_len + HALO, d_bc + n_heads), jnp.float32),
                        pltpu.VMEM((n_heads, seg_len), jnp.float32),
                        pltpu.VMEM((dests * PACK, LANES), jnp.float32),
                        pltpu.VMEM((n_prompts * CONV_WIDTH, d_bc), jnp.float32)],
        cost_estimate=pl.CostEstimate(flops=2 * m_rows * d_model * (d_bc + n_heads), bytes_accessed=2 * d_model * (d_bc + n_heads), transcendentals=0),
    )(h, halo, w_rows, conv_w, conv_b, dt_bias)


def x_kernel(layer, n_prompts, seg_len, d_inner, h_ref, halo_ref, dt_ref, w_ref, cw_ref, cb_ref, xs_ref,
             weights, arrived, h_ext, window, last_rows):
    step = pl.program_id(0)
    rows = n_prompts * seg_len
    tile = weights.shape[1]
    per = CONV_WIDTH

    @pl.when(step == 0)
    def _():
        start_weights(w_ref, layer, d_inner, tile, weights, arrived)
        h_ext[:rows] = h_ref[...]
        h_ext[rows:] = halo_ref[...]

    wait_weights(w_ref, layer, d_inner, tile, weights, arrived, step)
    fill_window(rounded_product(h_ext[...], weights[step]), window, n_prompts, seg_len)
    base = step * tile
    for prompt in range(n_prompts):
        last_rows[prompt * per:(prompt + 1) * per, :] = window[prompt, HALO + seg_len - per:, :]
    for block in range(tile // LANES):
        start = block * LANES
        for prompt in range(n_prompts):
            at = slice(prompt * seg_len, (prompt + 1) * seg_len)
            xs_ref[block, at, :] = convolve(window, cw_ref, cb_ref, prompt, seg_len, start, pl.multiple_of(base + start, LANES))
        dest = step * (tile // LANES) + block
        xs_ref[block, rows:rows + PACK, :] = dt_ref[pl.ds(pl.multiple_of(dest * PACK, PACK), PACK), :]
        xs_ref[block, rows + PACK:, :] = last_rows[:, start:start + LANES].astype(jnp.bfloat16)


def project_x(layer, h, halo, dt_all, w_rows, conv_w, conv_b, n_prompts, seg_len, d_inner):
    rows, d_model = h.shape
    tile = pick_tile(X_TILE, d_inner)
    steps = d_inner // tile
    per = tile // LANES
    m_rows = rows + halo.shape[0]
    sent_rows = rows + PACK + n_prompts * CONV_WIDTH
    whole = lambda *shape: pl.BlockSpec(shape, lambda s: (0,) * len(shape), pipeline_mode=pl.Buffered(1))
    return pl.pallas_call(
        functools.partial(x_kernel, layer, n_prompts, seg_len, d_inner),
        grid=(steps,),
        in_specs=[whole(*h.shape), whole(*halo.shape), whole(*dt_all.shape), pl.BlockSpec(memory_space=pl.ANY),
                  whole(*conv_w.shape), whole(*conv_b.shape)],
        out_specs=pl.BlockSpec((per, sent_rows, LANES), lambda s: (s, 0, 0)),
        out_shape=jax.ShapeDtypeStruct((d_inner // LANES, sent_rows, LANES), jnp.bfloat16),
        scratch_shapes=[pltpu.VMEM((steps, tile, d_model), jnp.bfloat16),
                        pltpu.SemaphoreType.DMA((steps,)),
                        pltpu.VMEM((m_rows, d_model), jnp.bfloat16),
                        pltpu.VMEM((n_prompts, seg_len + HALO, tile), jnp.float32),
                        pltpu.VMEM((n_prompts * CONV_WIDTH, tile), jnp.float32)],
        cost_estimate=pl.CostEstimate(flops=2 * m_rows * d_model * d_inner, bytes_accessed=2 * d_model * d_inner, transcendentals=0),
    )(h, halo, dt_all, w_rows, conv_w, conv_b)


def z_kernel(layer, h_ref, w_ref, z_ref, weights, arrived):
    step = pl.program_id(0)
    tile = weights.shape[1]

    @pl.when(step == 0)
    def _():
        start_weights(w_ref, layer, 0, tile, weights, arrived)

    wait_weights(w_ref, layer, 0, tile, weights, arrived, step)
    z_ref[...] = lax.dot_general(h_ref[...], weights[step], NT, preferred_element_type=jnp.float32).astype(jnp.bfloat16)


def project_z(layer, h, w_rows, d_inner):
    rows, d_model = h.shape
    tile = pick_tile(Z_TILE, d_inner)
    steps = d_inner // tile
    return pl.pallas_call(
        functools.partial(z_kernel, layer),
        grid=(steps,),
        in_specs=[pl.BlockSpec((rows, d_model), lambda s: (0, 0), pipeline_mode=pl.Buffered(1)),
                  pl.BlockSpec(memory_space=pl.ANY)],
        out_specs=pl.BlockSpec((rows, tile), lambda s: (0, s)),
        out_shape=jax.ShapeDtypeStruct((rows, d_inner), jnp.bfloat16),
        scratch_shapes=[pltpu.VMEM((steps, tile, d_model), jnp.bfloat16), pltpu.SemaphoreType.DMA((steps,))],
        cost_estimate=pl.CostEstimate(flops=2 * rows * d_model * d_inner, bytes_accessed=2 * d_model * d_inner, transcendentals=0),
    )(h, w_rows)


def scan_kernel(n_prompts, seg_len, segs, head_dim, d_state, x_ref, last_ref, bc_ref, a_ref, d_ref, y_ref, state_ref,
                row_refs, col_ref, dtc_ref):
    chunk = segs * seg_len
    rows = n_prompts * seg_len
    heads = LANES // head_dim

    @pl.when(pl.program_id(0) == 0)
    def _():
        state_ref[...] = jnp.zeros_like(state_ref)

    token_r = lax.broadcasted_iota(jnp.int32, (chunk, chunk), 0)
    token_c = lax.broadcasted_iota(jnp.int32, (chunk, chunk), 1)
    causal = token_r >= token_c
    lower = causal.astype(jnp.float32)
    upper = (token_r <= token_c).astype(jnp.float32)
    eye = (token_r == token_c).astype(jnp.float32)
    nt = (((1,), (1,)), ((), ()))
    tn = (((0,), (0,)), ((), ()))

    per_seg = [x_ref[seg, rows:rows + PACK, :].astype(jnp.float32)[:HALO] for seg in range(segs)]
    steps = jnp.concatenate([jnp.concatenate([part[:, head * seg_len:(head + 1) * seg_len] for part in per_seg], axis=1)
                             for head in range(heads)], axis=0)
    row_refs[...] = jnp.dot(steps, upper, preferred_element_type=jnp.float32)
    col_ref[...] = lax.dot_general(lower, steps, nt, preferred_element_type=jnp.float32)
    dtc_ref[...] = lax.dot_general(eye, steps, nt, preferred_element_type=jnp.float32)

    lane = lax.broadcasted_iota(jnp.int32, (chunk, LANES), 1)
    state_row = lax.broadcasted_iota(jnp.int32, (LANES, d_state), 0)
    pick = lax.broadcasted_iota(jnp.int32, (chunk, heads * HALO), 1)

    y_ref[:, rows:, :] = jnp.broadcast_to(last_ref[...], (segs,) + last_ref.shape[1:])

    @pl.loop(0, n_prompts, unroll=SCAN_UNROLL)
    def _(prompt):
        at = pl.ds(pl.multiple_of(prompt * seg_len, seg_len), seg_len)
        x_float = x_ref[:, at, :].reshape(chunk, LANES).astype(jnp.float32)
        b_part = bc_ref[:, 0, at, :d_state].reshape(chunk, d_state)
        c_part = bc_ref[:, 0, at, d_state:].reshape(chunk, d_state)
        scores = lax.dot_general(c_part, b_part, nt, preferred_element_type=jnp.float32)
        state = state_ref[prompt]
        y_inter = lax.dot_general(c_part.astype(jnp.float32), state, nt, preferred_element_type=jnp.float32)

        cums = [jnp.sum(jnp.where(pick == head * HALO + prompt, col_ref[...], 0.0), axis=1, keepdims=True) for head in range(heads)]
        dts = [jnp.sum(jnp.where(pick == head * HALO + prompt, dtc_ref[...], 0.0), axis=1, keepdims=True) for head in range(heads)]
        cum_log = jnp.broadcast_to(cums[0] * a_ref[0], (chunk, LANES))
        delta = jnp.broadcast_to(dts[0], (chunk, LANES))
        for head in range(1, heads):
            cum_log = jnp.where(lane >= head * head_dim, cums[head] * a_ref[head], cum_log)
            delta = jnp.where(lane >= head * head_dim, dts[head], delta)
        x_scaled = x_float * delta
        skip = jnp.broadcast_to(d_ref[0], (chunk, LANES))
        for head in range(1, heads):
            skip = jnp.where(lane >= head * head_dim, d_ref[head], skip)

        y_value = y_inter * jnp.exp(cum_log) + skip * x_float
        kept = jnp.zeros((LANES, d_state), jnp.float32)
        for head in range(heads):
            row = row_refs[pl.ds(head * HALO + prompt, 1), :]
            decay = jnp.exp(jnp.where(causal, (cums[head] - row) * a_ref[head], -jnp.inf))
            mine = (lane >= head * head_dim) & (lane < (head + 1) * head_dim)
            y_value = y_value + jnp.dot(decay * scores, jnp.where(mine, x_scaled, 0.0), preferred_element_type=jnp.float32)
            last = jnp.exp(cums[head][chunk - 1:chunk] * a_ref[head])
            kept = jnp.where(state_row >= head * head_dim, last, kept)
        x_left = x_scaled * jnp.exp(cum_log[chunk - 1:chunk] - cum_log)
        state_ref[prompt] = state * kept + lax.dot_general(x_left, b_part.astype(jnp.float32), tn, preferred_element_type=jnp.float32)
        y_ref[:, at, :] = y_value.astype(jnp.bfloat16).reshape(segs, seg_len, LANES)


def scan_heads(group, x_recv, bc_all, a_neg, d_vec, n_prompts, seg_len, head_dim, d_state):
    seg_count, rows_x, _ = x_recv.shape
    rows = n_prompts * seg_len
    heads = LANES // head_dim
    segs = 4
    while seg_count % segs:
        segs //= 2
    chunk = segs * seg_len
    steps = seg_count // segs
    n_last = n_prompts * CONV_WIDTH
    flops = steps * n_prompts * 2 * chunk * LANES * (chunk * (1 + heads) + 2 * d_state)
    return pl.pallas_call(
        functools.partial(scan_kernel, n_prompts, seg_len, segs, head_dim, d_state),
        grid=(steps,),
        in_specs=[pl.BlockSpec((segs, rows_x, LANES), lambda s: (s, 0, 0)),
                  pl.BlockSpec((1, n_last, LANES), lambda s: (seg_count - 1, rows_x // n_last - 1, 0)),
                  pl.BlockSpec((segs, 1, bc_all.shape[2], 2 * d_state), lambda s: (s, group, 0, 0)),
                  pl.BlockSpec(memory_space=pltpu.SMEM),
                  pl.BlockSpec(memory_space=pltpu.SMEM)],
        out_specs=[pl.BlockSpec((segs, rows + n_last, LANES), lambda s: (s, 0, 0)),
                   pl.BlockSpec((n_prompts, LANES, d_state), lambda s: (0, 0, 0))],
        out_shape=[jax.ShapeDtypeStruct((seg_count, rows + n_last, LANES), jnp.bfloat16),
                   jax.ShapeDtypeStruct((n_prompts, LANES, d_state), jnp.float32)],
        scratch_shapes=[pltpu.VMEM((heads * HALO, chunk), jnp.float32),
                        pltpu.VMEM((chunk, heads * HALO), jnp.float32),
                        pltpu.VMEM((chunk, heads * HALO), jnp.float32)],
        cost_estimate=pl.CostEstimate(flops=flops * 4, bytes_accessed=seg_count * rows * 2 * (2 * LANES + 2 * d_state), transcendentals=0),
    )(x_recv, x_recv, bc_all, a_neg, d_vec)


def out_kernel(layer, with_next, n_tiles, y_ref, z_ref, gate_ref, w_ref, resid_ref, pre_ref, *rest):
    if with_next:
        out_ref, h_ref, weights, arrived, normed, gated, kept = rest
    else:
        out_ref, weights, arrived, normed, gated = rest[-5:]
    step = pl.program_id(0)
    blocks = y_ref.shape[0]
    rows = z_ref.shape[0]
    part = gated.shape[0]
    tile = out_ref.shape[-1]

    def fetch(index):
        at = pl.ds(pl.multiple_of(index * tile, tile), tile)
        return pltpu.make_async_copy(w_ref.at[layer, :, at], weights.at[index], arrived.at[index])

    @pl.when(step == 0)
    def _():
        for index in range(n_tiles):
            fetch(index).start()

        @pl.loop(0, rows // part)
        def _(index):
            at = pl.ds(pl.multiple_of(index * part, part), part)
            total = jnp.zeros((part, LANES), jnp.float32)
            for block in range(blocks):
                lanes = slice(block * LANES, (block + 1) * LANES)
                value = y_ref[block, at, :].astype(jnp.float32) * silu(z_ref[at, lanes].astype(jnp.float32))
                total = total + value * value
                gated[:, lanes] = value
            mean_sq = jnp.sum(total, axis=1, keepdims=True) * (1.0 / (blocks * LANES))
            scale = lax.rsqrt(mean_sq + EPSILON)
            for block in range(blocks):
                lanes = slice(block * LANES, (block + 1) * LANES)
                normed[at, lanes] = (gated[:, lanes] * scale * gate_ref[:, lanes]).astype(jnp.bfloat16)

    fetch(step).wait()
    value = resid_ref[...] + jnp.dot(normed[...], weights[step], preferred_element_type=jnp.float32)
    out_ref[...] = value
    if with_next:
        kept[:, pl.ds(pl.multiple_of(step * tile, tile), tile)] = value

        @pl.when(step == n_tiles - 1)
        def _():
            @pl.loop(0, rows // part)
            def _(index):
                at = pl.ds(pl.multiple_of(index * part, part), part)
                row = kept[at, :]
                mean_sq = jnp.mean(row * row, axis=1, keepdims=True)
                h_ref[at, :] = (row * lax.rsqrt(mean_sq + EPSILON) * pre_ref[...]).astype(jnp.bfloat16)


def project_out(layer, y_recv, z, gate_w, w_out, resid, resid_block, next_pre, shared=None, out_block=0, out_rows=None):
    blocks, rows_y, _ = y_recv.shape
    rows = z.shape[0]
    d_inner = blocks * LANES
    d_model = resid.shape[-1]
    tile = pick_tile(OUT_TILE, d_model)
    n_tiles = d_model // tile
    with_next = next_pre is not None
    part = min(32, rows)
    whole = lambda *shape: pl.BlockSpec(shape, lambda s: (0,) * len(shape), pipeline_mode=pl.Buffered(1))
    out_specs = [pl.BlockSpec((rows, tile), lambda s: (out_block, s))]
    out_shape = [jax.ShapeDtypeStruct((out_rows or rows, d_model), jnp.float32)]
    scratch = [pltpu.VMEM((n_tiles, d_inner, tile), jnp.bfloat16), pltpu.SemaphoreType.DMA((n_tiles,)),
               pltpu.VMEM((rows, d_inner), jnp.bfloat16), pltpu.VMEM((part, d_inner), jnp.float32)]
    if with_next:
        out_specs.append(pl.BlockSpec((rows, d_model), lambda s: (0, 0)))
        out_shape.append(jax.ShapeDtypeStruct((rows, d_model), jnp.bfloat16))
        scratch.append(pltpu.VMEM((rows, d_model), jnp.float32))
    else:
        next_pre = gate_w[:, :d_model]
    extra = [] if shared is None else [shared]
    result = pl.pallas_call(
        functools.partial(out_kernel, layer, with_next, n_tiles),
        grid=(n_tiles,),
        in_specs=[whole(blocks, rows_y, LANES), whole(rows, d_inner), whole(1, d_inner),
                  pl.BlockSpec(memory_space=pl.ANY),
                  pl.BlockSpec((rows, tile), lambda s: (resid_block, s)), whole(1, d_model)] + [pl.BlockSpec(memory_space=pl.ANY)] * len(extra),
        input_output_aliases={6: 0} if extra else {},
        out_specs=out_specs,
        out_shape=out_shape,
        scratch_shapes=scratch,
        cost_estimate=pl.CostEstimate(flops=2 * rows * d_inner * d_model, bytes_accessed=2 * d_inner * d_model, transcendentals=0),
    )(y_recv, z, gate_w, w_out, resid, next_pre, *extra)
    return (result[0], result[1]) if with_next else (result[0], None)


def solution(mesh):
    seg_count = mesh.shape['sp']

    def step(resid, pre_norm, w_in, conv_w, conv_b, dt_bias, a_log, d_skip, gate_norm, w_out):
        batch, seg_len, d_model = resid.shape
        n_layers, n_groups, group_width = gate_norm.shape
        d_inner = n_groups * group_width
        n_heads = dt_bias.shape[1]
        conv_dim = conv_b.shape[1]
        d_bc = conv_dim - d_inner
        d_state = d_bc // (2 * n_groups)
        head_dim = d_inner // n_heads
        local_heads = n_heads // seg_count
        assert n_groups == 1 and local_heads * head_dim == LANES and seg_len * 2 == LANES
        seg_index = lax.axis_index('sp')
        n_prompts = batch // PROMPT_GROUPS
        rows = n_prompts * seg_len
        taps = jnp.swapaxes(conv_w, 1, 2)
        a_neg = -jnp.exp(lax.dynamic_slice_in_dim(a_log, seg_index * local_heads, local_heads, axis=1))
        d_local = lax.dynamic_slice_in_dim(d_skip, seg_index * local_heads, local_heads, axis=1)
        hops = [(source, source + 1) for source in range(seg_count - 1)]

        w_rows = jnp.swapaxes(w_in, 1, 2)
        whole_resid = resid.reshape(batch * seg_len, d_model)
        streams = []
        for group in range(PROMPT_GROUPS):
            part = whole_resid[group * rows:(group + 1) * rows]
            mean_sq = jnp.mean(part * part, axis=-1, keepdims=True)
            h = (part * lax.rsqrt(mean_sq + EPSILON) * pre_norm[0]).astype(jnp.bfloat16)
            streams.append((whole_resid, group, h))

        def exchange_halo(parts):
            edges = [h.reshape(n_prompts, seg_len, d_model)[:, seg_len - HALO:].reshape(n_prompts * HALO, d_model) for h in parts]
            halo = lax.ppermute(jnp.concatenate(edges, axis=0), 'sp', hops)
            return [halo[index * n_prompts * HALO:(index + 1) * n_prompts * HALO] for index in range(len(parts))]

        def gather(parts):
            return lax.all_gather(jnp.stack(parts, axis=0), 'sp', axis=0)

        groups = range(PROMPT_GROUPS)
        finals = []
        states = []
        for layer in range(n_layers):
            conv_args = (taps[layer], conv_b[layer][None, :])
            h_all = [item[2] for item in streams]
            if layer == 0:
                halos = exchange_halo(h_all)
            else:
                halos = [exchange_halo([h_all[group]])[0] for group in groups]
            bc_parts = []
            for group in groups:
                bc_parts.append(project_bc(layer, h_all[group], halos[group], w_rows, *conv_args, dt_bias[layer][None, :], n_prompts, seg_len, d_inner, d_bc))
            if layer == 0:
                bc_all = gather([item[0] for item in bc_parts])
                gathered = [(bc_all, group) for group in groups]
            else:
                gathered = [(gather([bc_parts[group][0]]), 0) for group in groups]
            arrived = []
            gates = []
            for group in groups:
                x_send = project_x(layer, h_all[group], halos[group], bc_parts[group][1], w_rows, *conv_args, n_prompts, seg_len, d_inner)
                arrived.append(lax.all_to_all(x_send, 'sp', 0, 0, tiled=True))
                gates.append(project_z(layer, h_all[group], w_rows, d_inner))
            next_streams = []
            layer_finals = []
            layer_tails = []
            shared = None
            for group in groups:
                part, block, _ = streams[group]
                bc_all, at = gathered[group]
                y_send, final = scan_heads(at, arrived[group], bc_all, a_neg[layer], d_local[layer], n_prompts, seg_len, head_dim, d_state)
                layer_finals.append(final.reshape(n_prompts, local_heads, head_dim, d_state))
                y_recv = lax.all_to_all(y_send, 'sp', 0, 0, tiled=True)
                x_tail = y_recv[:, rows:].reshape(-1, n_prompts, CONV_WIDTH, LANES)[:, :, 1:]
                x_tail = jnp.transpose(x_tail, (1, 0, 3, 2)).reshape(n_prompts, d_inner, CONV_WIDTH - 1)
                bc_tail = bc_all[seg_count - 1, at, rows:].reshape(n_prompts, CONV_WIDTH, d_bc)[:, 1:]
                layer_tails.append(jnp.concatenate([x_tail, jnp.swapaxes(bc_tail, 1, 2)], axis=1))
                if layer + 1 == n_layers:
                    shared, _ = project_out(layer, y_recv, gates[group], gate_norm[layer], w_out, part, block, None, shared, group, batch * seg_len)
                else:
                    new_part, new_h = project_out(layer, y_recv, gates[group], gate_norm[layer], w_out, part, block, pre_norm[layer + 1][None, :])
                    next_streams.append((new_part, 0, new_h))
            streams = next_streams
            finals.append(jnp.concatenate(layer_finals, axis=0))
            states.append(jnp.concatenate(layer_tails, axis=0))
        return shared.reshape(batch, seg_len, d_model), jnp.stack(finals, axis=1), jnp.stack(states, axis=1)

    return jax.shard_map(step, mesh=mesh, in_specs=(P('dp', 'sp', None), P(), P(), P(), P(), P(), P(), P(), P(), P()), out_specs=(P('dp', 'sp', None), P('dp', None, 'sp', None, None), P('dp', None, None, None)), check_vma=False)
```
